32 devices in a mesh: tm: 16 (over z, y, x), det: 2 (over core).
Axes of the slice: x: 2, y: 2, z: 4, core: 2. Of those that a mesh axis runs over, the one named last changes fastest.
Arguments:
- strain: float32 [2, 64, 192, 512], P('det', 'tm'), may hold values from -24 to 24
- final_half: float32 [2, 192, 512], P('det'), may hold values from -6 to 6
- intersection_function: float32 [16384], P('det'), may hold values from -1 to 1
- notch_mask: int32 [16384], P('det'), may hold values 0 or 1
- quality_flags: int32 [64], P('tm'), may hold values 0 or 1
Outputs:
- csd: float32 [64, 2, 16384], P('tm', None, 'det')
- stats: float32 [3, 64], P(None, 'tm')
- combined: float32 [2], replicated
The draws below stay inside these ranges and needn't reach their ends.
All inputs are finite; a program needn't handle non-finite values. No bound on the sum of `notch_mask` or of `quality_flags` on one device may be relied on, other than what follows from the above.
Results may differ from the reference program's by a relative error of at most 0.0003.
Values sent between devices are 32-bit elements; how exact they have to be, the bound alone decides.
No kernel may reach another device: no remote copies, remote signals or barrier semaphores. Data moves between devices by JAX's collectives and lax.ppermute only.
A program may use at most 64 MiB of HBM per device.

```python
import jax
import jax.numpy as jnp
from jax import lax

N2 = 512
K2 = 256
BIN = 6
SEGMENTS = 64
HALF_ROWS = 192
KC = 16384


def draw_strain(key, part):
    base_key = jax.random.fold_in(key, 11)
    noise_key, level_key = jax.random.split(base_key, 2)
    shape = (2, SEGMENTS, HALF_ROWS, N2)
    position = jnp.arange(SEGMENTS, dtype=jnp.float32) / SEGMENTS
    rough = jnp.exp(jax.random.uniform(level_key, (2, SEGMENTS), jnp.float32, jnp.log(0.7), jnp.log(1.4)))
    noise = jnp.clip(jax.random.normal(noise_key, shape, jnp.float32), -6.0, 6.0)
    trend = 3.0 ** (0.5 * position)
    values = noise * (trend[None, :] * rough)[:, :, None, None]
    return values.astype(jnp.float32)


def plant(result, key, least, high):
    index_at = [jax.random.randint(jax.random.fold_in(key, axis), (), 0, length) for axis, length in enumerate(result.shape)]
    widest = result.shape.index(max(result.shape))
    next_to = index_at[:widest] + [(index_at[widest] + 1) % result.shape[widest]] + index_at[widest + 1:]
    return result.at[tuple(index_at)].set(least).at[tuple(next_to)].set(high)


def steps_of(rng, dims, shards, least, top_value):
    def one(dim, blocks):
        draws = jax.random.uniform(jax.random.fold_in(jax.random.fold_in(rng, 6), dim), (blocks,), jnp.float32, least / len(shards), top_value / len(shards))
        return jnp.repeat(jnp.exp(draws), dims[dim] // blocks).reshape((-1,) + (1,) * (len(dims) - dim - 1))

    factor_of = one(*shards[0])
    for cut in shards[1:]:
        factor_of = factor_of * one(*cut)
    return factor_of


def gaussian(stream_key, extent, deviation, bound, cuts=(), held_as=jnp.bfloat16):
    array = jax.random.normal(stream_key, extent, jnp.float32) * deviation
    if len(cuts) > 0:
        array = steps_of(stream_key, extent, cuts, -0.22, 0.18) * array
    return jnp.clip(array, min=-bound, max=bound).astype(held_as)


def setup_inputs(seed: int = 0) -> dict:
    arg_keys = jax.random.split(jax.random.key(seed), 6)
    return {
        "strain": draw_strain(jax.random.fold_in(arg_keys[5], 71), 0),
        "final_half": gaussian(arg_keys[1], (2, HALF_ROWS, N2), 1.5, 6.0, ((0, 2),), jnp.float32),
        "intersection_function": jnp.clip(jax.random.uniform(arg_keys[2], (KC,), jnp.float32, -1.0, 1.0) * steps_of(arg_keys[2], (KC,), ((0, 2),), -0.4, 0.0), -1.0, 1.0),
        "notch_mask": plant((jax.random.randint(arg_keys[3], (KC,), 0, 8) < 7).astype(jnp.int32), jax.random.fold_in(arg_keys[3], 1), 0, 1),
        "quality_flags": plant((jax.random.randint(arg_keys[4], (SEGMENTS,), 0, 8) < 7).astype(jnp.int32), jax.random.fold_in(arg_keys[4], 1), 0, 1),
    }


INTERSECTION_CORR = 27.0 / 154.0

def reference(strain, final_half, intersection_function, notch_mask, quality_flags):
    segments = strain.shape[1]
    half_rows = strain.shape[2]
    columns = strain.shape[3]
    length = 2 * half_rows * columns
    fine_count = 2 * half_rows * K2
    sample_index = jnp.arange(length, dtype=jnp.int32).astype(jnp.float32)
    window = jnp.sin(jnp.pi * sample_index / length) ** 2
    scale_factor = (8.0 / (3.0 * length)) ** 0.5

    def spectra(segment_at):
        upper_half = lax.dynamic_index_in_dim(strain, segment_at, 1, keepdims=False)
        next_half = lax.dynamic_index_in_dim(strain, jnp.minimum(segment_at + 1, segments - 1).astype(jnp.int32), 1, keepdims=False)
        lower_half = jnp.where(segment_at + 1 < segments, next_half, final_half)
        windowed = jnp.concatenate([upper_half, lower_half], axis=1).reshape(2, length) * window
        fine_bins = jnp.fft.fft(windowed, axis=1)[:, :fine_count]
        part_real = fine_bins.real * scale_factor
        part_imag = fine_bins.imag * scale_factor
        cross_real = part_real[0] * part_real[1] + part_imag[0] * part_imag[1]
        cross_imag = part_real[0] * part_imag[1] - part_imag[0] * part_real[1]
        power = part_real * part_real + part_imag * part_imag
        cross_coarse = jnp.stack([cross_real, cross_imag]).reshape(2, fine_count // BIN, BIN).sum(axis=-1) / BIN
        power_coarse = power.reshape(2, fine_count // BIN, BIN).sum(axis=-1) / BIN
        return (cross_coarse, power_coarse)
    cross_coarse, power_coarse = lax.map(spectra, jnp.arange(segments, dtype=jnp.int32))
    coarse_bins = fine_count // BIN
    zero_row = jnp.zeros_like(power_coarse[:1])
    left_power = jnp.concatenate([zero_row, power_coarse[:-1]], axis=0)
    right_power = jnp.concatenate([power_coarse[1:], zero_row], axis=0)
    positions = jnp.arange(segments, dtype=jnp.int32)
    has_left = (positions > 0).astype(jnp.float32)[:, None, None]
    has_right = (positions < segments - 1).astype(jnp.float32)[:, None, None]
    mean_power = (has_left * left_power + has_right * right_power) / (has_left + has_right)
    filter_weight = notch_mask.astype(jnp.float32) * intersection_function / (mean_power[:, 0] * mean_power[:, 1])
    numerator = lax.optimization_barrier(jnp.sum(filter_weight * cross_coarse[:, 0], axis=-1))
    denominator = lax.optimization_barrier(jnp.sum(filter_weight * intersection_function, axis=-1))
    estimate = jnp.sqrt(12.0 * coarse_bins) * numerator / denominator
    spread = jnp.sqrt(coarse_bins / denominator)
    quality = quality_flags.astype(jnp.float32)
    tail_zero = jnp.zeros((1,), jnp.float32)
    up_next = jnp.concatenate([quality[1:] * spread[1:], tail_zero])
    down_next = jnp.concatenate([quality[1:] / spread[1:], tail_zero])
    covariance = INTERSECTION_CORR * quality * spread * up_next
    pair_term = INTERSECTION_CORR * quality / spread * down_next
    weight = quality / (spread * spread)
    weight_sum = jnp.sum(weight)
    weighted_sum = jnp.sum(weight * estimate)
    pair_sum = jnp.sum(pair_term)
    scale_root = jnp.sqrt(jnp.float32(segments))
    combined = scale_root * jnp.stack([weighted_sum / weight_sum, jnp.sqrt(weight_sum + 2.0 * pair_sum) / weight_sum])
    stats = jnp.stack([estimate, spread, covariance])
    return (cross_coarse, stats, combined)
```

```python
import functools

import jax
import jax.numpy as jnp
import numpy as np
from jax import lax
from jax.experimental import pallas as pl
from jax.experimental.pallas import tpu as pltpu
from jax.sharding import PartitionSpec as P

K2 = 256
BIN = 6
LANES = 128
SUB = 8
PAD = 16
WIDE = 256
DENOM_AT = 32
FLAG_AT = 64
INTERSECTION_CORR = 27.0 / 154.0
VMEM_LIMIT = 28 * 1024 * 1024


def halves_of(table):
    high = table.astype(jnp.bfloat16)
    low = (table - np.asarray(high, np.float64)).astype(jnp.bfloat16)
    return high, low


def tables(half_rows, columns, bands):
    full_rows = 2 * half_rows
    length = full_rows * columns
    groups = half_rows // BIN
    index = np.arange(half_rows)[:, None] * columns + np.arange(columns)[None, :]
    window = np.sin(np.pi * index / length) ** 2
    orders = []
    for parity in (0, 1):
        rows = []
        for r in range(parity, BIN, 2):
            rows.extend(BIN * j + r for j in range(groups))
            if r == 0:
                rows.extend([half_rows] * PAD)
        orders.append(np.array(rows))
    sections = []
    for rows in orders:
        k1 = half_rows + rows
        angle = 2.0 * np.pi / full_rows * (k1[:, None] * np.arange(half_rows)[None, :] % full_rows)
        sections.append(halves_of(np.concatenate([np.cos(angle), -np.sin(angle)], axis=0)))
    rows = np.concatenate(orders)
    angle = 2.0 * np.pi / length * (rows[:, None] * np.arange(columns)[None, :])
    twist = np.stack([np.cos(angle), np.sin(angle)]).astype(np.float32)
    width = K2 // bands
    per_row = LANES // (full_rows // BIN)
    seconds = []
    scale = (8.0 / (3.0 * length)) ** 0.5 / BIN**0.5
    for band in range(bands):
        block = band * width + np.arange(width).reshape(-1, per_row).T.reshape(-1)
        angle = np.pi / columns * (np.arange(columns)[:, None] * (2 * block + 1)[None, :] % (2 * columns))
        high, low = halves_of(scale * np.concatenate([np.cos(angle), np.sin(angle)], axis=1))
        seconds.append(np.concatenate([high, low], axis=1))
    return (
        window.astype(np.float32),
        np.concatenate(sections[0], axis=1),
        np.concatenate(sections[1], axis=1),
        twist,
        np.stack(seconds),
    )


def split(values):
    high = values.astype(jnp.bfloat16)
    return high, (values - high.astype(jnp.float32)).astype(jnp.bfloat16)


def product(high_one, low_one, high_two, low_two):
    dot = functools.partial(jnp.dot, preferred_element_type=jnp.float32)
    return dot(high_one, high_two) + dot(high_one, low_two) + dot(low_one, high_two)


def reversed_rows(values):
    order = (SUB - 1) - lax.broadcasted_iota(jnp.int32, (SUB, values.shape[1]), 0)
    parts = []
    for at in reversed(range(0, values.shape[0], SUB)):
        parts.append(jnp.take_along_axis(values[at : at + SUB], order, axis=0))
    return jnp.concatenate(parts, axis=0)


def natural(one, two):
    rows = one.shape[0]
    lane = lax.broadcasted_iota(jnp.int32, one.shape, 1)
    keep = lane < LANES // 2
    turned_one = pltpu.roll(one, LANES // 2, 1)
    turned_two = pltpu.roll(two, LANES // 2, 1)
    both = jnp.concatenate(
        [jnp.where(keep, one, turned_two), jnp.where(keep, turned_one, two)], axis=0
    ).T
    return both[:rows], both[rows:]


def transform(upper, lower, tabs, high, low, out):
    window, even, odd, twist, second = tabs
    half_rows, columns = window.shape
    even_rows, odd_rows = even.shape[0] // 2, odd.shape[0] // 2
    rows = even_rows + odd_rows
    for start in range(0, columns, WIDE):
        cols = slice(start, start + WIDE)
        shade = window[:, cols]
        first = upper(cols) * shade
        later = lower(cols)
        later = later - later * shade
        plus = split(first + later)
        minus = split(first - later)
        even_out = product(even[:, :half_rows], even[:, half_rows:], *plus)
        odd_out = product(odd[:, :half_rows], odd[:, half_rows:], *minus)
        for block, at, count in (
            (even_out, 0, even_rows),
            (odd_out, even_rows, odd_rows),
        ):
            real, imag = block[:count], block[count:]
            turn_cos = twist[0, at : at + count, cols]
            turn_sin = twist[1, at : at + count, cols]
            pair = split(real * turn_cos + imag * turn_sin)
            high[at : at + count, cols] = pair[0]
            low[at : at + count, cols] = pair[1]
            pair = split(imag * turn_cos - real * turn_sin)
            high[rows + at : rows + at + count, cols] = pair[0]
            low[rows + at : rows + at + count, cols] = pair[1]
    width = second.shape[1] // 2
    out[...] = product(high[...], low[...], second[:, :width], second[:, width:])


def correlate(spectra, rows, groups, imag_sign):
    starts = {}
    at = 0
    for parity in (0, 1):
        for r in range(parity, BIN, 2):
            starts[r] = at
            at += groups + (PAD if r == 0 else 0)
    starts[BIN] = starts[0] + 1
    straight = [0.0] * 4
    mirrored = [0.0] * 4
    for r in range(BIN + 1):
        loaded = []
        for det in range(2):
            top = spectra[det, pl.ds(starts[r], groups), :]
            bottom = spectra[det, pl.ds(rows + starts[r], groups), :]
            loaded.append((top[:, :LANES], top[:, LANES:], bottom[:, :LANES], bottom[:, LANES:]))
        for totals, sign, wanted in ((straight, 1.0, r < BIN), (mirrored, -1.0, r > 0)):
            if not wanted:
                continue
            parts = []
            for pc, ps, qc, qs in loaded:
                parts.append((pc + qs, qc - ps) if sign > 0 else (pc - qs, qc + ps))
            (real_one, imag_one), (real_two, imag_two) = parts
            totals[0] = totals[0] + (real_one * real_two + imag_one * imag_two)
            turn = real_one * imag_two - imag_one * real_two
            totals[1] = totals[1] + (turn if sign > 0 else -turn)
            totals[2] = totals[2] + (real_one * real_one + imag_one * imag_one)
            totals[3] = totals[3] + (real_two * real_two + imag_two * imag_two)
    planes = [jnp.concatenate([reversed_rows(b), a], axis=0) for a, b in zip(straight, mirrored)]
    planes[1] = planes[1] * imag_sign
    return natural(planes[0], planes[1]) + natural(planes[2], planes[3])


def put_csd(csd, real, imag):
    count = real.shape[0]
    csd[0, pl.ds(0, count, stride=2), :] = real
    csd[0, pl.ds(1, count, stride=2), :] = imag


def imag_sign_here():
    return jnp.where(lax.axis_index("det") == 0, 1.0, -1.0).astype(jnp.float32)


def early_kernel(
    mine_up, mine_low, other_up, other_low, window, even, odd, twist, second,
    csd, kept, message, high, low, spectra,
):
    tabs = (window, even, odd, twist, second)
    step = pl.program_id(0)
    rows = twist.shape[1]
    groups = window.shape[0] // BIN
    transform(lambda c: mine_up[0, :, c], lambda c: mine_low[0, :, c], tabs, high.at[0], low.at[0], spectra.at[0])
    transform(lambda c: other_up[0, :, c], lambda c: other_low[0, :, c], tabs, high.at[1], low.at[1], spectra.at[1])
    real, imag, power_one, power_two = correlate(spectra, rows, groups, imag_sign_here())
    put_csd(csd, real, imag)
    kept[0, 0] = power_one
    kept[0, 1] = power_two
    kept[0, 2] = real

    @pl.when(step == 0)
    def _():
        message[0] = power_one
        message[1] = power_two
        message[2] = real

    @pl.when(step == 1)
    def _():
        message[3] = power_one
        message[4] = power_two


def late_kernel(
    flags, mine_up, other_up, mine_next, other_next, mine_end, other_end, kept, ahead, weight, mask, csd_in,
    window, even, odd, twist, second,
    csd, sums, high, low, spectra,
):
    tabs = (window, even, odd, twist, second)
    rows = twist.shape[1]
    groups = window.shape[0] // BIN
    last = lax.axis_index("tm") == lax.axis_size("tm") - 1
    count = kept.shape[0] + 1

    def following(arrived, end):
        return lambda c: jnp.where(last, end[0, :, c], arrived[:, c])

    transform(lambda c: mine_up[0, :, c], following(mine_next, mine_end), tabs, high.at[0], low.at[0], spectra.at[0])
    transform(lambda c: other_up[0, :, c], following(other_next, other_end), tabs, high.at[1], low.at[1], spectra.at[1])
    real, imag, power_one, power_two = correlate(spectra, rows, groups, imag_sign_here())
    put_csd(csd, real, imag)
    powers = [(kept[s, 0], kept[s, 1]) for s in range(count - 1)]
    powers += [(power_one, power_two), (ahead[0], ahead[1]), (ahead[3], ahead[4])]
    reals = [kept[s, 2] for s in range(count - 1)] + [real, ahead[2]]
    overlap = weight[...]
    gain = mask[...].astype(jnp.float32) * overlap
    lane = lax.broadcasted_iota(jnp.int32, (1, LANES), 1)
    row = jnp.zeros((1, LANES), jnp.float32)
    for s in range(count + 1):
        if s == 0:
            mean_one, mean_two = powers[1]
        else:
            share = jnp.where(last, 1.0, 0.5) if s == count - 1 else 0.5
            mean_one = share * (powers[s - 1][0] + powers[s + 1][0])
            mean_two = share * (powers[s - 1][1] + powers[s + 1][1])
        filtered = gain / (mean_one * mean_two)
        for at, values in ((s, filtered * reals[s]), (DENOM_AT + s, filtered * overlap)):
            total = jnp.sum(jnp.sum(values, axis=0, keepdims=True), axis=1, keepdims=True)
            row = jnp.where(lane == at, total, row)
    for s in range(count):
        row = jnp.where(lane == FLAG_AT + s, 0.5 * flags[s].astype(jnp.float32), row)
    sums[...] = jnp.broadcast_to(row, sums.shape)


def final_kernel(count, coarse_bins, table, stats, combined, rows_of):
    chips = table.shape[0] // 2
    here = lax.axis_index("tm")
    both = table[pl.ds(0, chips, stride=2), :] + table[pl.ds(1, chips, stride=2), :]
    row = lax.broadcasted_iota(jnp.int32, both.shape, 0)
    lane = lax.broadcasted_iota(jnp.int32, both.shape, 1)

    def lanes_left(values, by):
        return pltpu.roll(values, (LANES - by) % LANES, 1)

    def in_place(values):
        moved = pltpu.roll(lanes_left(values, count), 1, 0)
        return jnp.where((lane == 0) & (row > 0), moved, values)

    def following(values):
        moved = pltpu.roll(pltpu.roll(values, chips - 1, 0), count - 1, 1)
        ahead = jnp.where(lane == count - 1, moved, lanes_left(values, 1))
        return jnp.where((lane == count - 1) & (row == chips - 1), 0.0, ahead)

    valid = lane < count
    numerator = jnp.where(valid, in_place(both), 0.0)
    denominator = jnp.where(valid, in_place(lanes_left(both, DENOM_AT)), 1.0)
    quality = jnp.where(valid, lanes_left(both, FLAG_AT), 0.0)
    spread = jnp.sqrt(coarse_bins / denominator)
    estimate = (12.0 * coarse_bins) ** 0.5 * numerator / denominator
    covariance = INTERSECTION_CORR * quality * spread * following(quality * spread)
    pair_term = INTERSECTION_CORR * quality / spread * following(quality / spread)
    weight = quality / (spread * spread)

    def total(values):
        return jnp.sum(jnp.sum(jnp.where(valid, values, 0.0), axis=0, keepdims=True), axis=1, keepdims=True)

    weight_sum, weighted_sum, pair_sum = total(weight), total(weight * estimate), total(pair_term)
    root = (chips * count) ** 0.5
    value = root * weighted_sum / weight_sum
    deviation = root * jnp.sqrt(weight_sum + 2.0 * pair_sum) / weight_sum
    two = lax.broadcasted_iota(jnp.int32, (1, LANES), 1)
    combined[...] = jnp.where(two == 0, value, deviation)[:, :2]
    for at, values in enumerate((estimate, spread, covariance)):
        rows_of[at] = values
        stats[at : at + 1, :] = rows_of[at, pl.ds(here, 1), :][:, :count]


def whole(array):
    return pl.BlockSpec(array.shape, lambda *_: (0,) * array.ndim)


def swapped(array):
    return lax.ppermute(array, "det", [(0, 1), (1, 0)])


def to_previous(array):
    return lax.ppermute(array, "tm", [(i, i - 1) for i in range(1, lax.axis_size("tm"))])


def on_device(consts, strain, final_half, intersection_function, notch_mask, quality_flags):
    halves = strain[0]
    count, half_rows, columns = halves.shape
    bands = lax.axis_size("det")
    devices = lax.axis_size("tm") * bands
    window, even, odd, twist, seconds = (jnp.asarray(c) for c in consts)
    arriving = to_previous(halves[0])
    other = swapped(halves)
    other_end = swapped(final_half)
    second = lax.dynamic_index_in_dim(seconds, lax.axis_index("det"), 0, keepdims=False)
    tabs = (window, even, odd, twist, second)
    bins = intersection_function.shape[0]
    plane = (bins // LANES, LANES)
    rows = twist.shape[1]
    scratch = [
        pltpu.VMEM((2, 2 * rows, columns), jnp.bfloat16),
        pltpu.VMEM((2, 2 * rows, columns), jnp.bfloat16),
        pltpu.VMEM((2, 2 * rows, 2 * LANES), jnp.float32),
    ]
    half = (1, half_rows, columns)
    csd_shape = (count, 2 * plane[0], LANES)
    flops = 2 * 2 * 3 * (2 * rows * half_rows * columns // 2 * 2 + 2 * rows * columns * 2 * LANES)
    params = pltpu.CompilerParams(vmem_limit_bytes=VMEM_LIMIT)
    csd, kept, message = pl.pallas_call(
        early_kernel,
        grid=(count - 1,),
        out_shape=(
            jax.ShapeDtypeStruct(csd_shape, jnp.float32),
            jax.ShapeDtypeStruct((count - 1, 3) + plane, jnp.float32),
            jax.ShapeDtypeStruct((5,) + plane, jnp.float32),
        ),
        in_specs=[
            pl.BlockSpec(half, lambda s: (s, 0, 0)),
            pl.BlockSpec(half, lambda s: (s + 1, 0, 0)),
            pl.BlockSpec(half, lambda s: (s, 0, 0)),
            pl.BlockSpec(half, lambda s: (s + 1, 0, 0)),
        ]
        + [whole(t) for t in tabs],
        out_specs=(
            pl.BlockSpec((1,) + csd_shape[1:], lambda s: (s, 0, 0)),
            pl.BlockSpec((1, 3) + plane, lambda s: (s, 0, 0, 0)),
            pl.BlockSpec((5,) + plane, lambda s: (0, 0, 0)),
        ),
        scratch_shapes=scratch,
        compiler_params=params,
        cost_estimate=pl.CostEstimate(
            flops=(count - 1) * flops, bytes_accessed=8 * 1024 * 1024, transcendentals=0
        ),
        name="early_segments",
    )(halves, halves, other, other, *tabs)
    ahead = to_previous(message)
    other_arriving = swapped(arriving)
    at_last = pl.BlockSpec(half, lambda _: (count - 1, 0, 0))
    csd, sums = pl.pallas_call(
        late_kernel,
        grid=(1,),
        out_shape=(
            jax.ShapeDtypeStruct(csd_shape, jnp.float32),
            jax.ShapeDtypeStruct((devices, LANES), jnp.float32),
        ),
        in_specs=[
            pl.BlockSpec(memory_space=pltpu.SMEM),
            at_last,
            at_last,
            whole(arriving),
            whole(other_arriving),
            whole(final_half),
            whole(other_end),
            whole(kept),
            whole(ahead),
            pl.BlockSpec(plane, lambda _: (0, 0)),
            pl.BlockSpec(plane, lambda _: (0, 0)),
            pl.BlockSpec(memory_space=pl.ANY),
        ]
        + [whole(t) for t in tabs],
        out_specs=(
            pl.BlockSpec((1,) + csd_shape[1:], lambda _: (count - 1, 0, 0)),
            pl.BlockSpec((devices, LANES), lambda _: (0, 0)),
        ),
        scratch_shapes=scratch,
        input_output_aliases={11: 0},
        compiler_params=params,
        cost_estimate=pl.CostEstimate(flops=flops, bytes_accessed=4 * 1024 * 1024, transcendentals=0),
        name="late_segment",
    )(
        quality_flags, halves, other, arriving, other_arriving, final_half, other_end, kept, ahead,
        intersection_function.reshape(plane), notch_mask.reshape(plane), csd, *tabs,
    )
    table = lax.all_to_all(sums, ("tm", "det"), 0, 0, tiled=True)
    stats, combined = pl.pallas_call(
        functools.partial(final_kernel, count, bins * bands),
        out_shape=(
            jax.ShapeDtypeStruct((3, count), jnp.float32),
            jax.ShapeDtypeStruct((1, 2), jnp.float32),
        ),
        scratch_shapes=[pltpu.VMEM((3, devices // bands, LANES), jnp.float32)],
        compiler_params=params,
        name="final_sums",
    )(table)
    cross = csd.reshape(count, plane[0], 2, LANES).transpose(0, 2, 1, 3).reshape(count, 2, bins)
    return cross, stats, combined.reshape(2)


def solution(mesh):
    def step(strain, final_half, intersection_function, notch_mask, quality_flags):
        consts = tables(strain.shape[2], strain.shape[3], mesh.shape["det"])
        return jax.shard_map(
            functools.partial(on_device, consts),
            mesh=mesh,
            in_specs=(P("det", "tm", None, None), P("det", None, None), P("det"), P("det"), P("tm")),
            out_specs=(P("tm", None, "det"), P(None, "tm"), P()),
            check_vma=False,
        )(strain, final_half, intersection_function, notch_mask, quality_flags)

    return step
```
